512 devices in a mesh: groups: 2 (over y), rows: 32 (over z), keys: 4 (over x), heads: 2 (over core).
Axes of the slice: x: 4, y: 2, z: 32, core: 2. Of those that a mesh axis runs over, the one named last changes fastest.
The devices are a block of a 4x8x32 slice.
Arguments:
- pair: bfloat16 [2048, 1024, 128], P(('groups', 'rows'), 'keys'), parts along dimension 0, may hold values from -6 to 6
- seq_length: int32 [2], P('groups'), parts along dimension 0, may hold values from 513 to 1024
- tile_counts: int32 [2048, 8], P(('groups', 'rows')), parts along dimension 0, may hold values from 0 to 128, as said below
- ln_gain: float32 [128], replicated, may hold values from 0.5 to 1.5
- w_query: bfloat16 [128, 128], P(None, 'heads'), may hold values from -8 to 8
- w_key: bfloat16 [128, 128], P(None, 'heads'), may hold values from -0.5 to 0.5
- w_value: bfloat16 [128, 128], P(None, 'heads'), may hold values from -0.5 to 0.5
- w_gate: bfloat16 [128, 128], P(None, 'heads'), may hold values from -0.5 to 0.5
- w_bias: bfloat16 [128, 4], P(None, 'heads'), may hold values from -1.5 to 1.5
- w_out: bfloat16 [128, 128], replicated, may hold values from -2 to 2
Outputs:
- update: bfloat16 [2048, 1024, 128], P(('groups', 'rows'), ('keys', 'heads')), parts along dimension 0
The draws below stay inside these ranges and needn't reach their ends.
There are 2 independent parts, one for each index of `groups`. The reference program is written for one: setup_inputs(seed, part) draws one part's arguments, and reference() takes and returns one part's arrays. A program takes and returns all parts, laid end to end along the dimension named above; an argument that names none is the same for every part. Nothing has to cross between parts.
Inputs may be any that keep to these rules, and one draw needn't show every extreme that they name: `tile_counts`: for each row and each tile of 128 keys, how many of the tile's leading keys are valid; some rows have no valid key at all.
All inputs are finite; a program needn't handle non-finite values.
Results may differ from the reference program's by a relative error of at most 0.03.
The reference program's roundings to bfloat16 on the way count: a program that leaves them out, or rounds other values in their place, can miss the bound.
Values may be sent and summed in bfloat16 or wider, within the bound.
A program may use at most 128 MiB of HBM per device.

```python
import jax
import jax.numpy as jnp
from jax import lax

C = 128
HEADS = 4
HEAD_DIM = 32
TILE = 128
L = 1024


def draw_tile_counts(key, part):
    first, second = jax.random.split(jax.random.fold_in(key, 11))
    counts = jax.random.randint(first, (L, L // TILE), 0, TILE + 1)
    keeper = jax.random.randint(second, (L, 1), 0, 8) > 0
    return jnp.where(keeper, counts, 0).astype(jnp.int32)


def draw_w_query(key, part):
    inner = jax.random.fold_in(key, 23)
    drawn = jnp.clip(jax.random.normal(inner, (C, HEADS * HEAD_DIM), jnp.float32), -4.0, 4.0) * C ** (-0.5)
    return drawn.astype(jnp.bfloat16)


def block_levels(stream_key, extent, cuts, least, top_value):
    def one(position, blocks):
        heights = jax.random.uniform(jax.random.fold_in(jax.random.fold_in(stream_key, 6), position), (blocks,), jnp.float32, least / len(cuts), top_value / len(cuts))
        return jnp.repeat(jnp.exp(heights), extent[position] // blocks).reshape((-1,) + (1,) * (len(extent) - position - 1))

    level = one(*cuts[0])
    for cut in cuts[1:]:
        level = level * one(*cut)
    return level


def centred(rng, extent, deviation, reach, cuts=(), kind=jnp.bfloat16):
    values = deviation * jax.random.normal(rng, extent, jnp.float32)
    if cuts:
        values = values * block_levels(rng, extent, cuts, -0.22, 0.18)
    return jnp.clip(values, -reach, reach).astype(kind)


def setup_inputs(seed: int = 0, part: int = 0) -> dict:
    streams_of = jax.random.split(jax.random.key(seed), 11)
    part_splits = jax.random.split(jax.random.fold_in(streams_of[10], part), 11)
    pair = centred(part_splits[0], (L, L, C), 1.0, 6.0, ((0, 32), (1, 4)))
    seq_length = jax.random.randint(part_splits[1], (1,), L // 2 + 1, L + 1).astype(jnp.int32)
    tile_counts = draw_tile_counts(jax.random.fold_in(jax.random.fold_in(streams_of[10], part), 71), part)
    ln_gain = jnp.clip(1.0 + 0.1 * jax.random.normal(streams_of[3], (C,), jnp.float32), 0.5, 1.5)
    w_query = draw_w_query(jax.random.fold_in(streams_of[10], 71), part)
    w_key = centred(streams_of[5], (C, HEADS * HEAD_DIM), C ** -0.5, 0.5, ((1, 2),))
    w_value = centred(streams_of[6], (C, HEADS * HEAD_DIM), C ** -0.5, 0.5, ((1, 2),))
    w_gate = centred(streams_of[7], (C, HEADS * HEAD_DIM), C ** -0.5, 0.5, ((1, 2),))
    w_bias = centred(streams_of[8], (C, HEADS), (C // 8) ** -0.5, 1.5, ((1, 2),))
    w_out = centred(streams_of[9], (HEADS * HEAD_DIM, C), (HEADS * HEAD_DIM // 16) ** -0.5, 2.0)
    return dict(pair=pair, seq_length=seq_length, tile_counts=tile_counts, ln_gain=ln_gain, w_query=w_query, w_key=w_key, w_value=w_value, w_gate=w_gate, w_bias=w_bias, w_out=w_out)


norm_epsilon = 1e-05
masked_score = -1e+30

def layer_norm(values, gain):
    center = values - lax.optimization_barrier(jnp.mean(values, axis=-1, keepdims=True))
    spread = lax.optimization_barrier(jnp.mean(center * center, axis=-1, keepdims=True))
    return center * lax.rsqrt(spread + norm_epsilon) * gain

def reference(pair, seq_length, tile_counts, ln_gain, w_query, w_key, w_value, w_gate, w_bias, w_out):
    width = HEADS * HEAD_DIM
    normed = layer_norm(pair.astype(jnp.float32), ln_gain).astype(jnp.bfloat16)
    flat = normed.reshape(L * L, C)
    queries = (jnp.dot(flat, w_query, preferred_element_type=jnp.float32) * HEAD_DIM ** (-0.5)).astype(jnp.bfloat16).reshape(L, L, HEADS, HEAD_DIM)
    keys_all = jnp.dot(flat, w_key, preferred_element_type=jnp.float32).astype(jnp.bfloat16).reshape(L, L, HEADS, HEAD_DIM)
    values_all = jnp.dot(flat, w_value, preferred_element_type=jnp.float32).astype(jnp.bfloat16).reshape(L, L, HEADS, HEAD_DIM)
    gate_act = jax.nn.sigmoid(jnp.dot(flat, w_gate, preferred_element_type=jnp.float32)).reshape(L, L, width)
    pair_bias = jnp.einsum('jkc,ch->hjk', normed.astype(jnp.float32), w_bias.astype(jnp.float32))
    positions = jnp.arange(L, dtype=jnp.int32)
    allowed = (positions[None, :] < seq_length[0]) & ((positions % TILE)[None, :] < jnp.repeat(tile_counts, TILE, axis=1))

    def one_row(operands):
        row_queries, row_keys, row_values, row_allowed = operands
        shown = row_allowed[None, None, :]
        scores = jnp.einsum('jhd,khd->hjk', row_queries.astype(jnp.float32), row_keys.astype(jnp.float32)) + pair_bias
        scores = jnp.where(shown, scores, masked_score)
        row_max = lax.optimization_barrier(jnp.max(scores, axis=-1, keepdims=True))
        weights = jnp.where(shown, jnp.exp(scores - row_max), 0.0)
        row_sum = lax.optimization_barrier(jnp.sum(weights, axis=-1))
        rounded = lax.optimization_barrier(weights.astype(jnp.bfloat16)).astype(jnp.float32)
        mixed = jnp.einsum('hjk,khd->jhd', rounded, row_values.astype(jnp.float32))
        denom = jnp.maximum(row_sum, 1.0)
        return (mixed / jnp.transpose(denom)[:, :, None]).astype(jnp.bfloat16)
    attended = lax.map(one_row, (queries, keys_all, values_all, allowed))
    attended = lax.optimization_barrier(attended.reshape(L, L, width)).astype(jnp.float32)
    gated = (gate_act * attended).astype(jnp.bfloat16)
    update = jnp.dot(gated.reshape(L * L, width), w_out, preferred_element_type=jnp.float32)
    return update.astype(jnp.bfloat16).reshape(L, L, C)
```

```python
import functools

import jax
import jax.numpy as jnp
from jax import lax
from jax.experimental import pallas as pl
from jax.experimental.pallas import tpu as pltpu
from jax.sharding import PartitionSpec as P

HEAD_DIM = 32
TILE = 128
norm_epsilon = 1e-05
masked_score = -1e30
CHUNKS = 8
MESH = pl.DeviceIdType.MESH
NT = (((1,), (1,)), ((), ()))
TN = (((0,), (0,)), ((), ()))


def nt(a, b):
    return lax.dot_general(a, b, NT, preferred_element_type=jnp.float32)


def exchange_kernel(
    pair_ref, gain_ref, wcat_ref, g_ref, bias_ref, wout_ref,
    xbuf, nbuf, wbuf, bpiece, bbuf,
    in_sem, w_send, w_recv, w_loc, b_send, b_recv, b_loc,
    z_recv, z_right, z_left,
    x_send, x_recv, y_send, y_recv, s_send, s_recv, g_loc, out_sem,
):
    x, c, r = lax.axis_index("keys"), lax.axis_index("heads"), lax.axis_index("rows")
    X, R = lax.axis_size("keys"), lax.axis_size("rows")
    rows, qdev, chan = nbuf.shape
    sources = bbuf.shape[0]
    pieces = 2 * X
    step = rows // CHUNKS
    half = step // 2
    mine = 2 * x + c
    xr, xl = lax.rem(x + 1, X), lax.rem(x + X - 1, X)
    zr, zl = lax.rem(r + 1, R), lax.rem(r + R - 1, R)
    sib = 1 - c

    load = pltpu.make_async_copy(pair_ref.at[:, pl.ds(pl.multiple_of(c * qdev, qdev), qdev), :], xbuf, in_sem)
    load.start()
    w_own = pltpu.make_async_copy(wcat_ref, wbuf.at[c], w_loc)
    w_own.start()

    barrier = pltpu.get_barrier_semaphore()
    for dx in range(X):
        for dc in range(2):
            if dx or dc:
                pl.semaphore_signal(
                    barrier, inc=1,
                    device_id={"keys": lax.rem(x + dx, X), "heads": lax.rem(c + dc, 2)},
                    device_id_type=MESH,
                )
    for z in (zr, zl):
        pl.semaphore_signal(barrier, inc=1, device_id={"rows": z}, device_id_type=MESH)
    pl.semaphore_wait(barrier, 2 * X - 1 + 2)

    def remote(src, dst, send, recv, where):
        return pltpu.make_async_remote_copy(
            src_ref=src, dst_ref=dst, send_sem=send, recv_sem=recv, device_id=where, device_id_type=MESH
        )

    w_copy = remote(wcat_ref, wbuf.at[c], w_send, w_recv, {"heads": sib})
    w_copy.start()
    load.wait()

    gain = gain_ref[...]

    def own_copies(m):
        at = pl.ds(m * step, step)
        src = nbuf.at[at]
        dst = g_ref.at[mine, at]
        return (
            remote(src, dst, x_send.at[0, m], x_recv.at[0, m], {"keys": xr}),
            remote(src, dst, x_send.at[1, m], x_recv.at[1, m], {"keys": xl}),
            remote(src, dst, x_send.at[2, m], x_recv.at[2, m], {"heads": sib}),
        )

    def send_own(m):
        for copy in own_copies(m):
            copy.start()
        pltpu.make_async_copy(nbuf.at[pl.ds(m * step, step)], g_ref.at[mine, pl.ds(m * step, step)], g_loc.at[m]).start()

    def norm_chunk(m, carry):
        at = pl.ds(m * step, step)
        v = xbuf[at].astype(jnp.float32)
        center = v - jnp.mean(v, axis=-1, keepdims=True)
        spread = jnp.mean(center * center, axis=-1, keepdims=True)
        nbuf[at] = (center * lax.rsqrt(spread + norm_epsilon) * gain[None]).astype(jnp.bfloat16)

        @pl.when(m > 0)
        def _():
            send_own(m - 1)

        return carry

    lax.fori_loop(0, CHUNKS, norm_chunk, 0)

    w_own.wait()
    w_copy.wait_recv()
    wb = jnp.concatenate([wbuf[0, 4], wbuf[1, 4]], axis=0).astype(jnp.float32)
    lane_row = lax.rem(lax.broadcasted_iota(jnp.int32, wb.shape, 0), rows)

    def bias_rows(n, acc):
        for k in range(4):
            j = n * 4 + k
            acc = acc + nt(nbuf[j], jnp.where(lane_row == j, wb, 0.0).astype(jnp.bfloat16))
        return acc

    acc = lax.fori_loop(0, rows // 4, bias_rows, jnp.zeros((qdev, 4 * rows), jnp.float32))
    bpiece[...] = acc.astype(jnp.bfloat16)
    send_own(CHUNKS - 1)

    block = (r * rows) // qdev
    a_me = lax.rem(r, sources)
    ox, oc = block // 2, lax.rem(block, 2)
    is_owner = block == mine

    def piece_at(a, p):
        return bbuf.at[a, pl.ds(p * qdev, qdev)]

    b_local = pltpu.make_async_copy(bpiece, piece_at(a_me, mine), b_loc)
    b_remote = remote(bpiece, piece_at(a_me, mine), b_send, b_recv.at[mine], {"keys": ox, "heads": oc})

    @pl.when(is_owner)
    def _():
        b_local.start()

    @pl.when(jnp.logical_not(is_owner))
    def _():
        b_remote.start()

    def to_right(a, p):
        return remote(piece_at(a, p), piece_at(a, p), z_right.at[a, p], z_recv.at[a, p], {"rows": zr})

    def to_left(a, p):
        return remote(piece_at(a, p), piece_at(a, p), z_left.at[a, p], z_recv.at[a, p], {"rows": zl})

    @pl.when(is_owner)
    def _():
        def own_piece(p, carry):
            @pl.when(p == mine)
            def _():
                b_local.wait()

            @pl.when(p != mine)
            def _():
                remote(bpiece, piece_at(a_me, p), b_send, b_recv.at[p], {"keys": ox, "heads": oc}).wait_recv()

            to_right(a_me, p).start()
            to_left(a_me, p).start()
            return carry

        lax.fori_loop(0, pieces, own_piece, 0)

    base = mine * sources
    middle = R // 2
    d0 = lax.rem(r - base + R, R)
    rightish = d0 <= middle + 1

    def place(n):
        t = n // pieces
        a = jnp.where(rightish, sources - 1 - t, t)
        return a, lax.rem(n, pieces), lax.rem(r - base - a + 2 * R, R)

    def z_time(n):
        _, _, d = place(n)
        hops = jnp.minimum(d, R - d)
        return 90 + 25 * hops + 7 * n

    def z_step(n):
        a, p, d = place(n)

        @pl.when(d != 0)
        def _():
            to_right(a, p).wait_recv()

            @pl.when(d < middle)
            def _():
                to_right(a, p).start()

            @pl.when(d > middle + 1)
            def _():
                to_left(a, p).start()

    left_piece, right_piece = 2 * xl + c, 2 * xr + c
    far_piece = 2 * lax.rem(x + 2, X) + c

    def forwards(m):
        lo, hi, at = pl.ds(m * step, half), pl.ds(m * step + half, half), pl.ds(m * step, step)
        return (
            remote(g_ref.at[left_piece, lo], g_ref.at[left_piece, lo], y_send.at[0, m], y_recv.at[0, m], {"keys": xr}),
            remote(g_ref.at[right_piece, hi], g_ref.at[right_piece, hi], y_send.at[1, m], y_recv.at[1, m], {"keys": xl}),
            remote(g_ref.at[left_piece, at], g_ref.at[left_piece, at], s_send.at[0, m], s_recv.at[0, m], {"heads": sib}),
            remote(g_ref.at[right_piece, at], g_ref.at[right_piece, at], s_send.at[1, m], s_recv.at[1, m], {"heads": sib}),
        )

    def far_copy(m):
        at = pl.ds(m * step, step)
        return remote(g_ref.at[far_piece, at], g_ref.at[far_piece, at], s_send.at[2, m], s_recv.at[2, m], {"heads": sib})

    def x_first(m):
        first, second, _ = own_copies(m)
        first.wait_recv()
        second.wait_recv()
        for copy in forwards(m):
            copy.start()

    def x_second(m):
        first, second, _, _ = forwards(m)
        first.wait_recv()
        second.wait_recv()
        far_copy(m).start()

    z_total = sources * pieces

    def x_time(n):
        return jnp.where(n < CHUNKS, 60 + 29 * (n + 1), 300 + 15 * (n - CHUNKS + 1))

    def merged(_, state):
        nz, nx = state
        use_x = jnp.logical_and(
            nx < 2 * CHUNKS, jnp.logical_or(nz >= z_total, x_time(nx) <= z_time(nz))
        )

        @pl.when(jnp.logical_and(use_x, nx < CHUNKS))
        def _():
            x_first(nx)

        @pl.when(jnp.logical_and(use_x, nx >= CHUNKS))
        def _():
            x_second(nx - CHUNKS)

        @pl.when(jnp.logical_not(use_x))
        def _():
            z_step(nz)

        took = use_x.astype(jnp.int32)
        return nz + 1 - took, nx + took

    lax.fori_loop(0, z_total + 2 * CHUNKS, merged, (0, 0))

    bias_out = pltpu.make_async_copy(bbuf, bias_ref, out_sem.at[0])
    w_out = pltpu.make_async_copy(wbuf, wout_ref, out_sem.at[1])
    bias_out.start()
    w_out.start()

    w_copy.wait_send()

    @pl.when(jnp.logical_not(is_owner))
    def _():
        b_remote.wait_send()

    def drain_z(n, carry):
        a, p, d = place(n)

        @pl.when(d < middle)
        def _():
            to_right(a, p).wait_send()

        @pl.when(jnp.logical_or(d == 0, d > middle + 1))
        def _():
            to_left(a, p).wait_send()

        return carry

    lax.fori_loop(0, z_total, drain_z, 0)

    def drain_x(m, carry):
        first, second, third = own_copies(m)
        for copy in (first, second, third):
            copy.wait_send()
        third.wait_recv()
        to_r, to_l, sib_l, sib_r = forwards(m)
        for copy in (to_r, to_l, sib_l, sib_r):
            copy.wait_send()
        sib_l.wait_recv()
        sib_r.wait_recv()
        far = far_copy(m)
        far.wait_send()
        far.wait_recv()
        pltpu.make_async_copy(nbuf.at[pl.ds(m * step, step)], g_ref.at[mine, pl.ds(m * step, step)], g_loc.at[m]).wait()
        return carry

    lax.fori_loop(0, CHUNKS, drain_x, 0)
    bias_out.wait()
    w_out.wait()


def exchange(pair, gain, wcat, key_groups, heads_axis):
    rows, cols, chan = pair.shape
    qdev = cols // heads_axis
    pieces = heads_axis * key_groups
    sources = qdev // rows
    length = qdev * pieces
    dma = pltpu.SemaphoreType.DMA
    any_spec = pl.BlockSpec(memory_space=pl.ANY)
    vmem = pl.BlockSpec(memory_space=pltpu.VMEM)
    bf16 = jnp.bfloat16
    return pl.pallas_call(
        exchange_kernel,
        name="exchange",
        out_shape=(
            jax.ShapeDtypeStruct((pieces, rows, qdev, chan), bf16),
            jax.ShapeDtypeStruct((sources, length, 4 * rows), bf16),
            jax.ShapeDtypeStruct((heads_axis, *wcat.shape), bf16),
        ),
        in_specs=[any_spec, vmem, vmem],
        out_specs=(any_spec, any_spec, any_spec),
        scratch_shapes=[
            pltpu.VMEM((rows, qdev, chan), bf16),
            pltpu.VMEM((rows, qdev, chan), bf16),
            pltpu.VMEM((heads_axis, *wcat.shape), bf16),
            pltpu.VMEM((qdev, 4 * rows), bf16),
            pltpu.VMEM((sources, length, 4 * rows), bf16),
            dma, dma, dma, dma, dma, dma((pieces,)), dma,
            dma((sources, pieces)), dma((sources, pieces)), dma((sources, pieces)),
            dma((3, CHUNKS)), dma((3, CHUNKS)), dma((2, CHUNKS)), dma((2, CHUNKS)),
            dma((3, CHUNKS)), dma((3, CHUNKS)), dma((CHUNKS,)), dma((2,)),
        ],
        compiler_params=pltpu.CompilerParams(collective_id=0, has_side_effects=True),
    )(pair, gain, wcat)


def attend_kernel(
    seq_ref, counts_ref, g_ref, bias_ref, w_ref, wout_ref, out_ref, bias32, keys_aug, q_bd
):
    i = pl.program_id(0)
    pieces, _, qdev, chan = g_ref.shape
    sources, length, lanes = bias_ref.shape
    rows = lanes // 4
    mine = 2 * lax.axis_index("keys") + lax.axis_index("heads")
    bf16, f32 = jnp.bfloat16, jnp.float32

    @pl.when(i == 0)
    def _():
        bias32[...] = bias_ref[...].astype(f32)
        q_bd[...] = jnp.zeros(q_bd.shape, bf16)
        first = lax.broadcasted_iota(jnp.int32, (16, sources * lanes), 0) == 0
        q_bd[chan:chan + 16, :] = jnp.where(first, 1.0, 0.0).astype(bf16)

    wq, wk, wv, wg = (jnp.concatenate([w_ref[0, k], w_ref[1, k]], axis=0) for k in range(4))
    rows_all = g_ref[...].reshape(length, chan)
    own = g_ref[mine, 0]

    keys_aug[:, :chan] = nt(rows_all, wk).astype(bf16)
    values_t = nt(wv, rows_all).astype(bf16)
    key_at = lax.broadcasted_iota(jnp.int32, (TILE, chan), 0)
    lane_at = lax.broadcasted_iota(jnp.int32, (TILE, chan), 1)
    for t in range(length // TILE):
        limit = jnp.minimum(counts_ref[i, t], seq_ref[0] - t * TILE)
        hit = jnp.logical_and(lane_at == 0, key_at >= limit)
        keys_aug[t * TILE:(t + 1) * TILE, chan:] = jnp.where(hit, masked_score, 0.0).astype(bf16)

    head_row = lax.broadcasted_iota(jnp.int32, (chan, lanes), 0) // HEAD_DIM
    head_lane = lax.broadcasted_iota(jnp.int32, (chan, lanes), 1) // rows
    diagonal = head_row == head_lane
    reps = [jnp.concatenate([own[a * rows:(a + 1) * rows]] * 4, axis=0) for a in range(sources)]
    for a in range(sources):
        qa = nt(wq, reps[a]) * HEAD_DIM ** (-0.5)
        q_bd[:chan, a * lanes:(a + 1) * lanes] = jnp.where(diagonal, qa, 0.0).astype(bf16)

    for b in range(sources // 2):
        cols = slice(2 * b * lanes, 2 * (b + 1) * lanes)
        scores = jnp.dot(keys_aug[...], q_bd[:, cols], preferred_element_type=f32)
        scores = scores + jnp.concatenate([bias32[2 * b], bias32[2 * b + 1]], axis=1)
        top = jnp.maximum(jnp.max(scores, axis=0, keepdims=True), masked_score * 0.1)
        weights = jnp.exp(scores - top)
        total = jnp.maximum(jnp.sum(weights, axis=0, keepdims=True), 1.0)
        mixed = jnp.dot(values_t, weights.astype(bf16), preferred_element_type=f32)
        attended = (mixed / total).astype(bf16).astype(f32)
        for k in range(2):
            a = 2 * b + k
            gate = jax.nn.sigmoid(nt(wg, reps[a]))
            gated = jnp.where(diagonal, gate * attended[:, k * lanes:(k + 1) * lanes], 0.0).astype(bf16)
            full = lax.dot_general(gated, wout_ref[...], TN, preferred_element_type=f32)
            summed = full[:rows] + full[rows:2 * rows] + full[2 * rows:3 * rows] + full[3 * rows:]
            out_ref[0, a * rows:(a + 1) * rows, :] = summed.astype(bf16)


def attend(seq_length, tile_counts, gathered, bias, weights, w_out):
    pieces, rows, qdev, chan = gathered.shape
    sources, length, lanes = bias.shape
    smem = pl.BlockSpec(memory_space=pltpu.SMEM)
    return pl.pallas_call(
        attend_kernel,
        name="attend",
        grid=(rows,),
        out_shape=jax.ShapeDtypeStruct((rows, qdev, chan), jnp.bfloat16),
        in_specs=[
            smem,
            smem,
            pl.BlockSpec((pieces, 1, qdev, chan), lambda i: (0, i, 0, 0)),
            pl.BlockSpec(bias.shape, lambda i: (0, 0, 0)),
            pl.BlockSpec(weights.shape, lambda i: (0, 0, 0, 0)),
            pl.BlockSpec(w_out.shape, lambda i: (0, 0)),
        ],
        out_specs=pl.BlockSpec((1, qdev, chan), lambda i: (i, 0, 0)),
        scratch_shapes=[
            pltpu.VMEM(bias.shape, jnp.float32),
            pltpu.VMEM((length, 2 * chan), jnp.bfloat16),
            pltpu.VMEM((2 * chan, sources * lanes), jnp.bfloat16),
        ],
    )(seq_length, tile_counts, gathered, bias, weights, w_out)


def per_device(
    pair, seq_length, tile_counts, ln_gain, w_query, w_key, w_value, w_gate, w_bias, w_out
):
    rows = pair.shape[0]
    bias_cols = jnp.repeat(w_bias, rows, axis=1)
    wcat = jnp.stack([w.T for w in (w_query, w_key, w_value, w_gate, bias_cols)])
    gathered, bias, weights = exchange(
        pair, ln_gain[None, :], wcat, lax.axis_size("keys"), lax.axis_size("heads")
    )
    return attend(seq_length, tile_counts, gathered, bias, weights, w_out)


def solution(mesh):
    in_specs = (
        P(("groups", "rows"), "keys", None),
        P("groups"),
        P(("groups", "rows"), None),
        P(),
        P(None, "heads"),
        P(None, "heads"),
        P(None, "heads"),
        P(None, "heads"),
        P(None, "heads"),
        P(),
    )
    out_specs = P(("groups", "rows"), ("keys", "heads"), None)
    return jax.shard_map(
        per_device, mesh=mesh, in_specs=in_specs, out_specs=out_specs, check_vma=False
    )
```
